16 devices in a mesh: rep: 1, dp: 16 (over x, y, z, core).
Axes of the slice: x: 2, y: 2, z: 2, core: 2. Of those that a mesh axis runs over, the one named last changes fastest.
Arguments:
- g_w_gate: bfloat16 [16, 2, 1280, 3584], P(('rep', 'dp'))
- g_w_up: bfloat16 [16, 2, 1280, 3584], P(('rep', 'dp'))
- g_w_down: bfloat16 [16, 2, 3584, 1280], P(('rep', 'dp'))
- w_gate: bfloat16 [2, 1280, 3584], replicated
- w_up: bfloat16 [2, 1280, 3584], replicated
- w_down: bfloat16 [2, 3584, 1280], replicated
- m_w_gate: float32 [2, 1280, 3584], P(None, 'dp')
- m_w_up: float32 [2, 1280, 3584], P(None, 'dp')
- m_w_down: float32 [2, 3584, 1280], P(None, 'dp')
- v_w_gate: float32 [2, 1280, 3584], P(None, 'dp')
- v_w_up: float32 [2, 1280, 3584], P(None, 'dp')
- v_w_down: float32 [2, 3584, 1280], P(None, 'dp')
Outputs:
- output 1: bfloat16 [2, 1280, 3584], P('rep')
- output 2: bfloat16 [2, 1280, 3584], P('rep')
- output 3: bfloat16 [2, 3584, 1280], P('rep')
- output 4: float32 [2, 1280, 3584], P('rep', 'dp')
- output 5: float32 [2, 1280, 3584], P('rep', 'dp')
- output 6: float32 [2, 3584, 1280], P('rep', 'dp')
- output 7: float32 [2, 1280, 3584], P('rep', 'dp')
- output 8: float32 [2, 1280, 3584], P('rep', 'dp')
- output 9: float32 [2, 3584, 1280], P('rep', 'dp')
All inputs are finite; a program needn't handle non-finite values.
Results may differ from the reference program's by a relative error of at most 0.022.
Values are sent between devices in bfloat16 or wider.
A program may use at most 2 GiB of HBM per device.

```python
import jax
import jax.numpy as jnp
from jax import lax

DEVICES = 16
D = 1280
FF = 3584
LAYERS = 2
NAMES = ("w_gate", "w_up", "w_down")
SHAPES = {"w_gate": (LAYERS, D, FF), "w_up": (LAYERS, D, FF), "w_down": (LAYERS, FF, D)}


def setup_inputs(seed: int = 0, part: int = 0) -> dict:
    kz, *keys = jax.random.split(jax.random.key(seed), 1 + 5 * len(NAMES))
    loud = 2.0 ** jax.random.uniform(kz, (), jnp.float32, -1.0, 1.0)
    drawn = {}
    for name, key, both in zip(NAMES, keys[:3], keys[3:6], strict=True):
        own = jax.random.normal(jax.random.fold_in(key, part), (DEVICES, *SHAPES[name]), jnp.float32)
        shared = jax.random.normal(jax.random.fold_in(both, part), SHAPES[name], jnp.float32)
        drawn["g_" + name] = (loud * (0.7 * shared / DEVICES + 0.7 * own * DEVICES**-0.5)).astype(jnp.bfloat16)
    for name, key in zip(NAMES, keys[6:9], strict=True):
        drawn[name] = (jax.random.normal(key, SHAPES[name], jnp.float32) * SHAPES[name][1] ** -0.5).astype(jnp.bfloat16)
    for name, key in zip(NAMES, keys[9:12], strict=True):
        drawn["m_" + name] = loud * 0.5 * jax.random.normal(key, SHAPES[name], jnp.float32)
    for name, key in zip(NAMES, keys[12:15], strict=True):
        drawn["v_" + name] = loud * loud * jax.random.uniform(key, SHAPES[name], jnp.float32, 0.5, 1.5)
    return drawn


def adamw(w, m, v, g):
    m = 0.9 * m + 0.1 * g
    v = 0.95 * v + 0.05 * g * g
    step = m * lax.rsqrt(v + 1e-8) + 0.1 * w
    return (w - 0.02 * step).astype(jnp.bfloat16), m, v


def clipped(gradients, sum_of_squares, count):
    factor = jnp.minimum(1.0, 0.5 * lax.rsqrt(sum_of_squares / count + 1e-30))
    return [g * factor for g in gradients]


def reference(g_w_gate, g_w_up, g_w_down, w_gate, w_up, w_down, m_w_gate, m_w_up, m_w_down, v_w_gate, v_w_up, v_w_down):
    def total(terms):
        return lax.scan(lambda so_far, term: (so_far + term.astype(jnp.float32), None), jnp.zeros(terms.shape[1:], jnp.float32), terms)[0]

    gradients = [total(terms).astype(jnp.bfloat16).astype(jnp.float32) for terms in (g_w_gate, g_w_up, g_w_down)]
    gradients = clipped(gradients, sum(jnp.sum(g * g) for g in gradients), sum(g.size for g in gradients))
    new = [
        adamw(w.astype(jnp.float32), m, v, g)
        for w, m, v, g in zip((w_gate, w_up, w_down), (m_w_gate, m_w_up, m_w_down), (v_w_gate, v_w_up, v_w_down), gradients, strict=True)
    ]
    return tuple(one[which] for which in range(3) for one in new)
```

```python
import jax
import jax.numpy as jnp
from jax import lax
from jax.experimental import pallas as pl
from jax.experimental.pallas import tpu as pltpu
from jax.sharding import PartitionSpec as P

MESH = pl.DeviceIdType.MESH
F32, BF16 = jnp.float32, jnp.bfloat16
LAYERS = 2
PARTS = 14
WAVES = LAYERS * PARTS
SLOTS = 8
AHEAD = 3
ORDERS = ((0, 1, 2), (1, 2, 0), (2, 0, 1))
BITS = (8, 4, 2)


def flip(me, bit):
    return me + bit * (1 - 2 * ((me // bit) % 2))


class Weight:
    def __init__(self, k, rows, columns):
        self.k, self.rows, self.columns = k, rows, columns
        self.by_columns = columns > rows * 8
        self.shape = (rows, columns // PARTS) if self.by_columns else (rows // PARTS, columns)
        self.axes = ORDERS[k]
        self.rest = tuple(sorted(self.axes[1:]))

    def part(self, wave):
        layer, cut = wave // PARTS, wave % PARTS
        if self.by_columns:
            wide = self.shape[1]
            return layer, (slice(None), pl.ds(pl.multiple_of(cut * wide, wide), wide))
        tall = self.shape[0]
        return layer, (pl.ds(pl.multiple_of(cut * tall, tall), tall), slice(None))


def where(fixed):
    return tuple(fixed.get(axis, slice(None)) for axis in range(3))


def kernel(weights, count, *refs):
    it = iter(refs)
    take = lambda: [next(it) for _ in weights]
    g_in, w_in, m_in, v_in = take(), take(), take(), take()
    w_out, m_out, v_out = take(), take(), take()
    own, other, first, second, third = take(), take(), take(), take(), take()
    g_own, w_own, m_own, v_own, squares = take(), take(), take(), take(), take()
    part_sum, all_sums = next(it), next(it)
    (load_sem, die_send, die_recv, send_sem, recv_sem, gather_send, gather_recv, back_send, back_recv, local_sem, state_sem, sum_send, sum_recv, credit) = it

    me = lax.axis_index("dp")
    core = me % 2
    at = tuple((me // bit) % 2 for bit in BITS)
    near = tuple(flip(me, bit) for bit in BITS)
    twin = flip(me, 1)

    def remote(src, dst, send, recv, device):
        return pltpu.make_async_remote_copy(src_ref=src, dst_ref=dst, send_sem=send, recv_sem=recv, device_id={"dp": device}, device_id_type=MESH)

    def load(w, wave):
        layer, cut = w.part(wave)
        slot = wave % SLOTS
        return pltpu.make_async_copy(g_in[w.k].at[(layer, slice(None), slice(None), slice(None), core, *cut)], own[w.k].at[slot], load_sem.at[slot, w.k])

    def swap(w, wave):
        layer, cut = w.part(wave)
        slot = wave % SLOTS
        src = g_in[w.k].at[(layer, slice(None), slice(None), slice(None), 1 - core, *cut)]
        return remote(src, other[w.k].at[slot], die_send.at[slot, w.k], die_recv.at[slot, w.k], twin)

    def away(w, stage):
        fixed = {axis: at[axis] for axis in w.axes[:stage]}
        fixed[w.axes[stage]] = 1 - at[w.axes[stage]]
        return fixed

    def pass_on(w, wave, stage):
        slot = wave % SLOTS
        src = own[w.k].at[(slot, *where(away(w, stage)))]
        dst = (first, second, third)[stage][w.k].at[slot]
        return remote(src, dst, send_sem.at[slot, stage, w.k], recv_sem.at[slot, stage, w.k], near[w.axes[stage]])

    def total(w, slot, block, stage):
        so_far = own[w.k][(slot, *block)].astype(F32) + other[w.k][(slot, *block)].astype(F32)
        if stage > 0:
            so_far += first[w.k][(slot, *(block[axis] for axis in w.rest))].astype(F32)
        if stage > 1:
            so_far += second[w.k][slot, block[w.axes[2]]].astype(F32)
        if stage > 2:
            so_far += third[w.k][slot].astype(F32)
        return so_far

    def sum_and_pass(w, wave, stage):
        slot = wave % SLOTS
        fixed = away(w, stage)
        free = [axis for axis in range(3) if axis not in fixed]

        @pl.loop(0, 2 ** len(free))
        def _(i):
            block = dict(fixed)
            for n, axis in enumerate(free):
                block[axis] = (i // 2**n) % 2
            block = tuple(block[axis] for axis in range(3))
            own[w.k][(slot, *block)] = total(w, slot, block, stage).astype(BF16)

        pass_on(w, wave, stage).start()

    def finish(w, wave):
        layer, cut = w.part(wave)
        g = total(w, wave % SLOTS, at, 3).astype(BF16)
        g_own[w.k][(layer, *cut)] = g
        g = g.astype(F32)
        g = g * g
        squares[w.k][...] += sum(g[8 * i : 8 * i + 8] for i in range(w.shape[0] // 8))

    def state_copies():
        copies = []
        for w in weights:
            copies += [
                pltpu.make_async_copy(m_in[w.k], m_own[w.k], state_sem.at[0, w.k]),
                pltpu.make_async_copy(v_in[w.k], v_own[w.k], state_sem.at[1, w.k]),
                pltpu.make_async_copy(w_in[w.k].at[(slice(None), *at, core)], w_own[w.k], state_sem.at[2, w.k]),
            ]
        return copies

    def state_out():
        copies = []
        for w in weights:
            copies += [
                pltpu.make_async_copy(m_own[w.k], m_out[w.k], state_sem.at[3, w.k]),
                pltpu.make_async_copy(v_own[w.k], v_out[w.k], state_sem.at[4, w.k]),
            ]
        return copies

    for w in weights:
        for wave in range(AHEAD):
            load(w, wave).start()
    for w in weights:
        squares[w.k][...] = jnp.zeros_like(squares[w.k])

    barrier = pltpu.get_barrier_semaphore()
    for k in range(1, 16):
        pl.semaphore_signal(barrier, inc=1, device_id={"dp": (me + k) % 16}, device_id_type=MESH)
    pl.semaphore_wait(barrier, 15)

    for wave in range(AHEAD):
        for w in weights:
            swap(w, wave).start()
    for copy in state_copies():
        copy.start()

    def drain(wave):
        for w in weights:
            swap(w, wave).wait_send()
            for stage in range(3):
                pass_on(w, wave, stage).wait_send()

    @pl.loop(0, WAVES + 3)
    def _(step):
        @pl.when(step < WAVES)
        def _():
            for w in weights:
                load(w, step).wait()
                swap(w, step).wait_recv()
                sum_and_pass(w, step, 0)

        @pl.when(step + AHEAD < WAVES)
        def _():
            wave = step + AHEAD

            @pl.when(wave >= SLOTS)
            def _():
                drain(wave - SLOTS)
                pl.semaphore_wait(credit, 1)

            for w in weights:
                load(w, wave).start()
                swap(w, wave).start()

        for stage in (1, 2):

            @pl.when((step >= stage) & (step - stage < WAVES))
            def _():
                for w in weights:
                    pass_on(w, step - stage, stage - 1).wait_recv()
                    sum_and_pass(w, step - stage, stage)

        @pl.when(step >= 3)
        def _():
            for w in weights:
                pass_on(w, step - 3, 2).wait_recv()
                finish(w, step - 3)

            @pl.when(step - 3 + SLOTS < WAVES)
            def _():
                pl.semaphore_signal(credit, inc=1, device_id={"dp": twin}, device_id_type=MESH)

    @pl.loop(WAVES - SLOTS, WAVES)
    def _(wave):
        drain(wave)

    mine = jnp.zeros((8, 128), F32)
    for w in weights:
        for i in range(w.shape[1] // 128):
            mine += squares[w.k][:, 128 * i : 128 * i + 128]
    part_sum[...] = mine

    def tell(k):
        return remote(part_sum, all_sums.at[k - 1], sum_send.at[k - 1], sum_recv.at[k - 1], (me + k) % 16)

    for k in range(1, 16):
        tell(k).start()
    for copy in state_copies():
        copy.wait()
    sums = mine
    for k in range(1, 16):
        tell(k).wait_recv()
        sums += all_sums[k - 1]
    sums = jnp.sum(jnp.sum(sums, axis=0, keepdims=True), axis=1, keepdims=True)
    factor = jnp.minimum(1.0, 0.5 * lax.rsqrt(sums / count + 1e-30))

    def update(w, wave):
        layer, cut = w.part(wave)
        here = (layer, *cut)
        g = g_own[w.k][here].astype(F32) * factor
        m = 0.9 * m_own[w.k][here] + 0.1 * g
        v = 0.95 * v_own[w.k][here] + 0.05 * g * g
        weight = w_own[w.k][here].astype(F32)
        w_own[w.k][here] = (weight - 0.02 * (m * lax.rsqrt(v + 1e-8) + 0.1 * weight)).astype(BF16)
        m_own[w.k][here] = m
        v_own[w.k][here] = v

    def out_at(w, wave, fixed, which):
        layer, cut = w.part(wave)
        return w_out[w.k].at[(layer, *where(fixed), which, *cut)]

    def keep(w, wave):
        layer, cut = w.part(wave)
        return pltpu.make_async_copy(w_own[w.k].at[(layer, *cut)], out_at(w, wave, dict(enumerate(at)), core), local_sem.at[wave % SLOTS, w.k])

    def give(w, wave, stage):
        slot = wave % SLOTS
        axes = w.axes[::-1]
        dst = out_at(w, wave, {axis: at[axis] for axis in axes[stage:]}, core)
        layer, cut = w.part(wave)
        src = w_own[w.k].at[(layer, *cut)] if stage == 0 else dst
        return remote(src, dst, gather_send.at[slot, stage, w.k], gather_recv.at[slot, stage, w.k], near[axes[stage]])

    def give_twin(w, wave, half):
        slot = wave % SLOTS
        axis = w.axes[0]
        side = at[axis] if half == 0 else 1 - at[axis]
        ref = out_at(w, wave, {axis: side}, core)
        return remote(ref, ref, back_send.at[slot, half, w.k], back_recv.at[slot, half, w.k], twin)

    @pl.loop(0, WAVES + 7)
    def _(step):
        @pl.when(step < WAVES)
        def _():
            for w in weights:
                update(w, step)
                give(w, step, 0).start()
                keep(w, step).start()

        @pl.when((step >= 1) & (step - 1 < WAVES))
        def _():
            for w in weights:
                keep(w, step - 1).wait()
                give(w, step - 1, 0).wait_recv()
                give(w, step - 1, 1).start()

        @pl.when((step >= 2) & (step - 2 < WAVES))
        def _():
            for w in weights:
                give(w, step - 2, 1).wait_recv()
                give(w, step - 2, 2).start()
                give_twin(w, step - 2, 0).start()

        @pl.when((step >= 3) & (step - 3 < WAVES))
        def _():
            for w in weights:
                give(w, step - 3, 2).wait_recv()
                give_twin(w, step - 3, 1).start()

        @pl.when((step >= 5) & (step - 5 < WAVES))
        def _():
            for w in weights:
                for half in range(2):
                    give_twin(w, step - 5, half).wait_recv()

        @pl.when((step >= 7) & (step - 7 < WAVES))
        def _():
            for w in weights:
                for stage in range(3):
                    give(w, step - 7, stage).wait_send()
                for half in range(2):
                    give_twin(w, step - 7, half).wait_send()

        @pl.when(step == WAVES)
        def _():
            for copy in state_out():
                copy.start()

    for copy in state_out():
        copy.wait()
    for k in range(1, 16):
        tell(k).wait_send()


def solution(mesh):
    def step(*arrays):
        terms, whole, m, v = (arrays[i : i + 3] for i in (0, 3, 6, 9))
        weights = [Weight(k, *one.shape[1:]) for k, one in enumerate(m)]
        count = 16 * sum(one.size for one in m)
        cut = [(LAYERS, 2, 2, 2, 2, w.rows, w.columns) for w in weights]
        held = lambda n, extra=(): [pltpu.VMEM((n, *extra, *w.shape), BF16) for w in weights]
        block = lambda dtype: [pltpu.VMEM((LAYERS, w.rows, w.columns), dtype) for w in weights]
        scratch = (
            held(SLOTS, (2, 2, 2))
            + held(SLOTS, (2, 2, 2))
            + held(SLOTS, (2, 2))
            + held(SLOTS, (2,))
            + held(SLOTS)
            + block(BF16)
            + block(BF16)
            + block(F32)
            + block(F32)
            + [pltpu.VMEM((8, w.shape[1]), F32) for w in weights]
            + [pltpu.VMEM((8, 128), F32), pltpu.VMEM((15, 8, 128), F32)]
            + [pltpu.SemaphoreType.DMA((SLOTS, 3))] * 3
            + [pltpu.SemaphoreType.DMA((SLOTS, 3, 3))] * 4
            + [pltpu.SemaphoreType.DMA((SLOTS, 2, 3))] * 2
            + [pltpu.SemaphoreType.DMA((SLOTS, 3)), pltpu.SemaphoreType.DMA((5, 3))]
            + [pltpu.SemaphoreType.DMA((15,))] * 2
            + [pltpu.SemaphoreType.REGULAR]
        )
        anywhere = pl.BlockSpec(memory_space=pl.ANY)
        out = pl.pallas_call(
            lambda *refs: kernel(weights, float(count), *refs),
            out_shape=[jax.ShapeDtypeStruct(c, BF16) for c in cut] + [jax.ShapeDtypeStruct(one.shape, F32) for one in (*m, *v)],
            in_specs=[anywhere] * 12,
            out_specs=[anywhere] * 9,
            scratch_shapes=scratch,
            compiler_params=pltpu.CompilerParams(collective_id=0, has_side_effects=True, vmem_limit_bytes=60 * 2**20),
            name="step",
        )(*(t.reshape(c) for t, c in zip(terms, cut)), *(t.reshape(c) for t, c in zip(whole, cut)), *m, *v)
        return (*(o.reshape(t.shape) for o, t in zip(out[:3], whole)), *out[3:])

    all_of, cut = P(None, None, None), P(None, "dp", None)
    return jax.shard_map(
        step,
        mesh=mesh,
        in_specs=(P(("rep", "dp"), None, None, None),) * 3 + (all_of,) * 3 + (cut,) * 6,
        out_specs=(P("rep", None, None),) * 3 + (P("rep", "dp", None),) * 6,
        check_vma=False,
    )
```

```python
import jax
import jax.numpy as jnp
from jax import lax
from jax.experimental import pallas as pl
from jax.experimental.pallas import tpu as pltpu
from jax.sharding import PartitionSpec as P

MESH = pl.DeviceIdType.MESH
F32, BF16 = jnp.float32, jnp.bfloat16
LAYERS = 2
PARTS = 14
WAVES = LAYERS * PARTS
SLOTS = 8
HELD = 6
RING = 4
ROOM = 32
GRANT = 8 * 2**20
AHEAD = 3
ORDERS = ((0, 1, 2), (1, 2, 0), (2, 0, 1))
BITS = (8, 4, 2)


def flip(me, bit):
    return me + bit * (1 - 2 * ((me // bit) % 2))


class Weight:
    def __init__(self, k, rows, columns):
        self.k, self.rows, self.columns = k, rows, columns
        self.by_columns = columns > rows * 8
        self.shape = (rows, columns // PARTS) if self.by_columns else (rows // PARTS, columns)
        self.axes = ORDERS[k]
        self.rest = tuple(sorted(self.axes[1:]))

    def part(self, wave):
        layer, cut = wave // PARTS, wave % PARTS
        if self.by_columns:
            wide = self.shape[1]
            return layer, (slice(None), pl.ds(pl.multiple_of(cut * wide, wide), wide))
        tall = self.shape[0]
        return layer, (pl.ds(pl.multiple_of(cut * tall, tall), tall), slice(None))


def where(fixed):
    return tuple(fixed.get(axis, slice(None)) for axis in range(3))


def kernel(weights, count, *refs):
    it = iter(refs)
    take = lambda: [next(it) for _ in weights]
    g_in, w_in, m_in, v_in = take(), take(), take(), take()
    w_out, state_out = take(), take()
    first, second, third = take(), take(), take()
    w_own, m_own, v_own, squares = take(), take(), take(), take()
    part_sum, all_sums = next(it), next(it)
    (load_sem, die_send, die_recv, send_sem, recv_sem, gather_send, gather_recv, back_send, back_recv, state_sem, sum_send, sum_recv) = it

    me = lax.axis_index("dp")
    core = me % 2
    at = tuple((me // bit) % 2 for bit in BITS)
    near = tuple(flip(me, bit) for bit in BITS)
    twin = flip(me, 1)

    def remote(src, dst, send, recv, device):
        return pltpu.make_async_remote_copy(src_ref=src, dst_ref=dst, send_sem=send, recv_sem=recv, device_id={"dp": device}, device_id_type=MESH)

    def load(w, wave):
        layer, cut = w.part(wave)
        spot = (layer, slice(None), slice(None), slice(None), core, *cut)
        return pltpu.make_async_copy(g_in[w.k].at[spot], w_out[w.k].at[spot], load_sem.at[wave % SLOTS, w.k])

    def swap(w, wave):
        layer, cut = w.part(wave)
        slot = wave % SLOTS
        src = g_in[w.k].at[(layer, slice(None), slice(None), slice(None), 1 - core, *cut)]
        dst = w_out[w.k].at[(layer, slice(None), slice(None), slice(None), core, *cut)]
        return remote(src, dst, die_send.at[slot, w.k], die_recv.at[slot, w.k], twin)

    def away(w, stage):
        fixed = {axis: at[axis] for axis in w.axes[:stage]}
        fixed[w.axes[stage]] = 1 - at[w.axes[stage]]
        return fixed

    def pass_on(w, wave, stage):
        layer, cut = w.part(wave)
        src = w_out[w.k].at[(layer, *where(away(w, stage)), core, *cut)]
        dst = (first, second, third)[stage][w.k].at[wave % HELD]
        send, recv = send_sem.at[wave % SLOTS, stage, w.k], recv_sem.at[wave % HELD, stage, w.k]
        return remote(src, dst, send, recv, near[w.axes[stage]])

    def total(w, wave, block, stage):
        layer, cut = w.part(wave)
        slot = wave % HELD
        so_far = w_out[w.k][(layer, *block, core, *cut)].astype(F32) + w_out[w.k][(layer, *block, 1 - core, *cut)].astype(F32)
        if stage > 0:
            so_far += first[w.k][(slot, *(block[axis] for axis in w.rest))].astype(F32)
        if stage > 1:
            so_far += second[w.k][slot, block[w.axes[2]]].astype(F32)
        if stage > 2:
            so_far += third[w.k][slot].astype(F32)
        return so_far

    def sum_and_pass(w, wave, stage):
        layer, cut = w.part(wave)
        fixed = away(w, stage)
        free = [axis for axis in range(3) if axis not in fixed]

        @pl.loop(0, 2 ** len(free))
        def _(i):
            block = dict(fixed)
            for n, axis in enumerate(free):
                block[axis] = (i // 2**n) % 2
            block = tuple(block[axis] for axis in range(3))
            w_out[w.k][(layer, *block, core, *cut)] = total(w, wave, block, stage).astype(BF16)

        pass_on(w, wave, stage).start()

    def finish(w, wave):
        layer, cut = w.part(wave)
        g = total(w, wave, at, 3).astype(BF16)
        w_out[w.k][(layer, *at, core, *cut)] = g
        g = g.astype(F32)
        g = g * g
        squares[w.k][...] += sum(g[8 * i : 8 * i + 8] for i in range(w.shape[0] // 8))

    def fetch(w, wave):
        layer, cut = w.part(wave)
        slot = wave % RING
        return (
            pltpu.make_async_copy(m_in[w.k].at[(layer, *cut)], m_own[w.k].at[slot], state_sem.at[slot, 0, w.k]),
            pltpu.make_async_copy(v_in[w.k].at[(layer, *cut)], v_own[w.k].at[slot], state_sem.at[slot, 1, w.k]),
            pltpu.make_async_copy(w_in[w.k].at[(layer, *at, core, *cut)], w_own[w.k].at[slot], state_sem.at[slot, 2, w.k]),
        )

    def put(w, wave):
        layer, cut = w.part(wave)
        slot = wave % RING
        return (
            pltpu.make_async_copy(m_own[w.k].at[slot], state_out[w.k].at[(0, layer, *cut)], state_sem.at[slot, 3, w.k]),
            pltpu.make_async_copy(v_own[w.k].at[slot], state_out[w.k].at[(1, layer, *cut)], state_sem.at[slot, 4, w.k]),
        )

    for wave in range(AHEAD):
        for w in weights:
            load(w, wave).start()
    for w in weights:
        squares[w.k][...] = jnp.zeros_like(squares[w.k])

    barrier = pltpu.get_barrier_semaphore()
    for k in range(1, 16):
        pl.semaphore_signal(barrier, inc=1, device_id={"dp": (me + k) % 16}, device_id_type=MESH)
    pl.semaphore_wait(barrier, 15)

    for wave in range(AHEAD):
        for w in weights:
            swap(w, wave).start()
    for wave in range(RING):
        for w in weights:
            for copy in fetch(w, wave):
                copy.start()

    def drain(wave):
        for w in weights:
            swap(w, wave).wait_send()
            for stage in range(3):
                pass_on(w, wave, stage).wait_send()

    @pl.loop(0, WAVES + 3)
    def _(step):
        @pl.when(step < WAVES)
        def _():
            for w in weights:
                load(w, step).wait()
                swap(w, step).wait_recv()
                sum_and_pass(w, step, 0)

        @pl.when(step + AHEAD < WAVES)
        def _():
            wave = step + AHEAD

            @pl.when(wave >= SLOTS)
            def _():
                drain(wave - SLOTS)

            for w in weights:
                load(w, wave).start()
                swap(w, wave).start()

        for stage in (1, 2):

            @pl.when((step >= stage) & (step - stage < WAVES))
            def _():
                for w in weights:
                    pass_on(w, step - stage, stage - 1).wait_recv()
                    sum_and_pass(w, step - stage, stage)

        @pl.when(step >= 3)
        def _():
            for w in weights:
                pass_on(w, step - 3, 2).wait_recv()
                finish(w, step - 3)

    @pl.loop(WAVES - SLOTS, WAVES)
    def _(wave):
        drain(wave)

    mine = jnp.zeros((8, 128), F32)
    for w in weights:
        for i in range(w.shape[1] // 128):
            mine += squares[w.k][:, 128 * i : 128 * i + 128]
    part_sum[...] = mine

    def tell(k):
        return remote(part_sum, all_sums.at[k - 1], sum_send.at[k - 1], sum_recv.at[k - 1], (me + k) % 16)

    for k in range(1, 16):
        tell(k).start()
    sums = mine
    for k in range(1, 16):
        tell(k).wait_recv()
        sums += all_sums[k - 1]
    sums = jnp.sum(jnp.sum(sums, axis=0, keepdims=True), axis=1, keepdims=True)
    factor = jnp.minimum(1.0, 0.5 * lax.rsqrt(sums / count + 1e-30))

    def update(w, wave):
        layer, cut = w.part(wave)
        here = (layer, *at, core, *cut)
        slot = wave % RING
        g = w_out[w.k][here].astype(F32) * factor
        m = 0.9 * m_own[w.k][slot] + 0.1 * g
        v = 0.95 * v_own[w.k][slot] + 0.05 * g * g
        weight = w_own[w.k][slot].astype(F32)
        w_out[w.k][here] = (weight - 0.02 * (m * lax.rsqrt(v + 1e-8) + 0.1 * weight)).astype(BF16)
        m_own[w.k][slot] = m
        v_own[w.k][slot] = v

    def out_at(w, wave, fixed, which):
        layer, cut = w.part(wave)
        return w_out[w.k].at[(layer, *where(fixed), which, *cut)]

    def give(w, wave, stage):
        slot = wave % SLOTS
        axes = w.axes[::-1]
        ref = out_at(w, wave, {axis: at[axis] for axis in axes[stage:]}, core)
        return remote(ref, ref, gather_send.at[slot, stage, w.k], gather_recv.at[slot, stage, w.k], near[axes[stage]])

    def give_twin(w, wave, half):
        slot = wave % SLOTS
        axis = w.axes[0]
        side = at[axis] if half == 0 else 1 - at[axis]
        ref = out_at(w, wave, {axis: side}, core)
        return remote(ref, ref, back_send.at[slot, half, w.k], back_recv.at[slot, half, w.k], twin)

    @pl.loop(0, WAVES + 7)
    def _(step):
        @pl.when(step < WAVES)
        def _():
            for w in weights:
                for copy in fetch(w, step):
                    copy.wait()
                update(w, step)
                give(w, step, 0).start()
                for copy in put(w, step):
                    copy.start()

        @pl.when((step >= 1) & (step - 1 < WAVES))
        def _():
            for w in weights:
                give(w, step - 1, 0).wait_recv()
                give(w, step - 1, 1).start()

        @pl.when((step >= 2) & (step - 2 < WAVES))
        def _():
            for w in weights:
                give(w, step - 2, 1).wait_recv()
                give(w, step - 2, 2).start()
                give_twin(w, step - 2, 0).start()

        @pl.when((step >= 3) & (step - 3 < WAVES))
        def _():
            for w in weights:
                give(w, step - 3, 2).wait_recv()
                give_twin(w, step - 3, 1).start()

        @pl.when((step >= 2) & (step - 2 < WAVES))
        def _():
            for w in weights:
                for copy in put(w, step - 2):
                    copy.wait()

        @pl.when((step >= 2) & (step + 2 < WAVES))
        def _():
            for w in weights:
                for copy in fetch(w, step + 2):
                    copy.start()

        @pl.when((step >= 5) & (step - 5 < WAVES))
        def _():
            for w in weights:
                for half in range(2):
                    give_twin(w, step - 5, half).wait_recv()

        @pl.when((step >= 7) & (step - 7 < WAVES))
        def _():
            for w in weights:
                for stage in range(3):
                    give(w, step - 7, stage).wait_send()
                for half in range(2):
                    give_twin(w, step - 7, half).wait_send()

    for k in range(1, 16):
        tell(k).wait_send()


def hand_over(w_from, state, w_to, m_to, v_to, m_by, v_by, sem):
    inward = [pltpu.make_async_copy(state.at[0], m_by, sem.at[0]), pltpu.make_async_copy(state.at[1], v_by, sem.at[1])]
    outward = [pltpu.make_async_copy(m_by, m_to, sem.at[0]), pltpu.make_async_copy(v_by, v_to, sem.at[1])]
    cuts = [(layer, x) for layer in range(LAYERS) for x in range(2)]
    weight = [pltpu.make_async_copy(w_from.at[cut], w_to.at[cut], sem.at[2 + n]) for n, cut in enumerate(cuts)]
    for copy in inward + weight:
        copy.start()
    for copy, back in zip(inward, outward):
        copy.wait()
        back.start()
    for copy in outward + weight:
        copy.wait()


def solution(mesh):
    def step(*arrays):
        terms, whole, m, v = (arrays[i : i + 3] for i in (0, 3, 6, 9))
        weights = [Weight(k, *one.shape[1:]) for k, one in enumerate(m)]
        count = 16 * sum(one.size for one in m)
        cut = [(LAYERS, 2, 2, 2, 2, w.rows, w.columns) for w in weights]
        held = lambda n, extra=(), dtype=BF16: [pltpu.VMEM((n, *extra, *w.shape), dtype) for w in weights]
        scratch = (
            held(HELD, (2, 2))
            + held(HELD, (2,))
            + held(HELD)
            + held(RING)
            + held(RING, dtype=F32)
            + held(RING, dtype=F32)
            + [pltpu.VMEM((8, w.shape[1]), F32) for w in weights]
            + [pltpu.VMEM((8, 128), F32), pltpu.VMEM((15, 8, 128), F32)]
            + [pltpu.SemaphoreType.DMA((SLOTS, 3))] * 3
            + [pltpu.SemaphoreType.DMA((SLOTS, 3, 3))] * 4
            + [pltpu.SemaphoreType.DMA((SLOTS, 2, 3))] * 2
            + [pltpu.SemaphoreType.DMA((RING, 5, 3))]
            + [pltpu.SemaphoreType.DMA((15,))] * 2
        )
        anywhere = pl.BlockSpec(memory_space=pl.ANY)
        out = pl.pallas_call(
            lambda *refs: kernel(weights, float(count), *refs),
            out_shape=[pltpu.VMEM(c, BF16) for c in cut] + [jax.ShapeDtypeStruct((ROOM, *one.shape), F32) for one in m],
            in_specs=[anywhere] * 12,
            out_specs=[pl.BlockSpec(memory_space=pltpu.VMEM)] * 3 + [anywhere] * 3,
            scratch_shapes=scratch,
            compiler_params=pltpu.CompilerParams(collective_id=0, has_side_effects=True, vmem_limit_bytes=GRANT),
            name="step",
        )(*(t.reshape(c) for t, c in zip(terms, cut)), *(t.reshape(c) for t, c in zip(whole, cut)), *m, *v)
        new = [
            pl.pallas_call(
                hand_over,
                out_shape=[jax.ShapeDtypeStruct(cut[w.k], BF16)] + [jax.ShapeDtypeStruct(m[w.k].shape, F32)] * 2,
                in_specs=[pl.BlockSpec(memory_space=pltpu.VMEM), anywhere],
                out_specs=[anywhere] * 3,
                scratch_shapes=[pltpu.VMEM(m[w.k].shape, F32)] * 2 + [pltpu.SemaphoreType.DMA((6,))],
                compiler_params=pltpu.CompilerParams(vmem_limit_bytes=5 * 2**20),
                name="hand_over",
            )(*out[w.k :: 3])
            for w in weights
        ]
        return (*(one[0].reshape(t.shape) for one, t in zip(new, whole)), *(one[1] for one in new), *(one[2] for one in new))

    all_of, cut = P(None, None, None), P(None, "dp", None)
    return jax.shard_map(
        step,
        mesh=mesh,
        in_specs=(P(("rep", "dp"), None, None, None),) * 3 + (all_of,) * 3 + (cut,) * 6,
        out_specs=(P("rep", None, None),) * 3 + (P("rep", "dp", None),) * 6,
        check_vma=False,
    )
```

```python
import jax
import jax.numpy as jnp
from jax import lax
from jax.experimental import pallas as pl
from jax.experimental.pallas import tpu as pltpu
from jax.sharding import PartitionSpec as P

MESH = pl.DeviceIdType.MESH
F32, BF16 = jnp.float32, jnp.bfloat16
LAYERS = 2
PARTS = 14
WAVES = LAYERS * PARTS
SLOTS = 8
HELD = 6
RING = 6
ROOM = 32
GRANT = 9 * 2**20
LEAD = 3
AHEAD = 3
ORDERS = ((0, 1, 2), (1, 2, 0), (2, 0, 1))
BITS = (8, 4, 2)


def flip(me, bit):
    return me + bit * (1 - 2 * ((me // bit) % 2))


class Weight:
    def __init__(self, k, rows, columns):
        self.k, self.rows, self.columns = k, rows, columns
        self.by_columns = columns > rows * 8
        self.shape = (rows, columns // PARTS) if self.by_columns else (rows // PARTS, columns)
        self.axes = ORDERS[k]
        self.rest = tuple(sorted(self.axes[1:]))

    def part(self, wave):
        layer, cut = wave // PARTS, wave % PARTS
        if self.by_columns:
            wide = self.shape[1]
            return layer, (slice(None), pl.ds(pl.multiple_of(cut * wide, wide), wide))
        tall = self.shape[0]
        return layer, (pl.ds(pl.multiple_of(cut * tall, tall), tall), slice(None))


def where(fixed):
    return tuple(fixed.get(axis, slice(None)) for axis in range(3))


def kernel(weights, count, *refs):
    it = iter(refs)
    take = lambda: [next(it) for _ in weights]
    g_in, w_in, m_in, v_in = take(), take(), take(), take()
    w_out, state_out = take(), take()
    first, second, third = take(), take(), take()
    w_own, m_own, v_own, squares = take(), take(), take(), take()
    part_sum, all_sums = next(it), next(it)
    (load_sem, die_send, die_recv, send_sem, recv_sem, gather_send, gather_recv, back_send, back_recv, state_sem, sum_send, sum_recv) = it

    me = lax.axis_index("dp")
    core = me % 2
    at = tuple((me // bit) % 2 for bit in BITS)
    near = tuple(flip(me, bit) for bit in BITS)
    twin = flip(me, 1)

    def remote(src, dst, send, recv, device):
        return pltpu.make_async_remote_copy(src_ref=src, dst_ref=dst, send_sem=send, recv_sem=recv, device_id={"dp": device}, device_id_type=MESH)

    def load(w, wave):
        layer, cut = w.part(wave)
        spot = (layer, slice(None), slice(None), slice(None), core, *cut)
        return pltpu.make_async_copy(g_in[w.k].at[spot], w_out[w.k].at[spot], load_sem.at[wave % SLOTS, w.k])

    def swap(w, wave):
        layer, cut = w.part(wave)
        slot = wave % SLOTS
        src = g_in[w.k].at[(layer, slice(None), slice(None), slice(None), 1 - core, *cut)]
        dst = w_out[w.k].at[(layer, slice(None), slice(None), slice(None), core, *cut)]
        return remote(src, dst, die_send.at[slot, w.k], die_recv.at[slot, w.k], twin)

    def away(w, stage):
        fixed = {axis: at[axis] for axis in w.axes[:stage]}
        fixed[w.axes[stage]] = 1 - at[w.axes[stage]]
        return fixed

    def pass_on(w, wave, stage):
        layer, cut = w.part(wave)
        src = w_out[w.k].at[(layer, *where(away(w, stage)), core, *cut)]
        dst = (first, second, third)[stage][w.k].at[wave % HELD]
        send, recv = send_sem.at[wave % SLOTS, stage, w.k], recv_sem.at[wave % HELD, stage, w.k]
        return remote(src, dst, send, recv, near[w.axes[stage]])

    def total(w, wave, block, stage):
        layer, cut = w.part(wave)
        slot = wave % HELD
        so_far = w_out[w.k][(layer, *block, core, *cut)].astype(F32) + w_out[w.k][(layer, *block, 1 - core, *cut)].astype(F32)
        if stage > 0:
            so_far += first[w.k][(slot, *(block[axis] for axis in w.rest))].astype(F32)
        if stage > 1:
            so_far += second[w.k][slot, block[w.axes[2]]].astype(F32)
        if stage > 2:
            so_far += third[w.k][slot].astype(F32)
        return so_far

    def sum_and_pass(w, wave, stage):
        layer, cut = w.part(wave)
        fixed = away(w, stage)
        free = [axis for axis in range(3) if axis not in fixed]

        @pl.loop(0, 2 ** len(free))
        def _(i):
            block = dict(fixed)
            for n, axis in enumerate(free):
                block[axis] = (i // 2**n) % 2
            block = tuple(block[axis] for axis in range(3))
            w_out[w.k][(layer, *block, core, *cut)] = total(w, wave, block, stage).astype(BF16)

        pass_on(w, wave, stage).start()

    def finish(w, wave):
        layer, cut = w.part(wave)
        g = total(w, wave, at, 3).astype(BF16)
        w_out[w.k][(layer, *at, core, *cut)] = g
        g = g.astype(F32)
        g = g * g
        squares[w.k][...] += sum(g[8 * i : 8 * i + 8] for i in range(w.shape[0] // 8))

    def fetch(w, wave):
        layer, cut = w.part(wave)
        slot = wave % RING
        return (
            pltpu.make_async_copy(m_in[w.k].at[(layer, *cut)], m_own[w.k].at[slot], state_sem.at[slot, 0, w.k]),
            pltpu.make_async_copy(v_in[w.k].at[(layer, *cut)], v_own[w.k].at[slot], state_sem.at[slot, 1, w.k]),
            pltpu.make_async_copy(w_in[w.k].at[(layer, *at, core, *cut)], w_own[w.k].at[slot], state_sem.at[slot, 2, w.k]),
        )

    def put(w, wave):
        layer, cut = w.part(wave)
        slot = wave % RING
        return (
            pltpu.make_async_copy(m_own[w.k].at[slot], state_out[w.k].at[(0, layer, *cut)], state_sem.at[slot, 3, w.k]),
            pltpu.make_async_copy(v_own[w.k].at[slot], state_out[w.k].at[(1, layer, *cut)], state_sem.at[slot, 4, w.k]),
        )

    for wave in range(AHEAD):
        for w in weights:
            load(w, wave).start()
    for w in weights:
        squares[w.k][...] = jnp.zeros_like(squares[w.k])

    barrier = pltpu.get_barrier_semaphore()
    for k in range(1, 16):
        pl.semaphore_signal(barrier, inc=1, device_id={"dp": (me + k) % 16}, device_id_type=MESH)
    pl.semaphore_wait(barrier, 15)

    for wave in range(AHEAD):
        for w in weights:
            swap(w, wave).start()
    def drain(wave):
        for w in weights:
            swap(w, wave).wait_send()
            for stage in range(3):
                pass_on(w, wave, stage).wait_send()

    @pl.loop(0, WAVES + 3)
    def _(step):
        @pl.when(step >= 4)
        def _():
            drain(step - 4)

        @pl.when(step < WAVES)
        def _():
            for w in weights:
                load(w, step).wait()
                swap(w, step).wait_recv()
                sum_and_pass(w, step, 0)

        @pl.when(step + AHEAD < WAVES)
        def _():
            for w in weights:
                load(w, step + AHEAD).start()
                swap(w, step + AHEAD).start()

        @pl.when((step >= SLOTS) & (step < SLOTS + RING))
        def _():
            for w in weights:
                for copy in fetch(w, step - SLOTS):
                    copy.start()

        for stage in (1, 2):

            @pl.when((step >= stage) & (step - stage < WAVES))
            def _():
                for w in weights:
                    pass_on(w, step - stage, stage - 1).wait_recv()
                    sum_and_pass(w, step - stage, stage)

        @pl.when(step >= 3)
        def _():
            for w in weights:
                pass_on(w, step - 3, 2).wait_recv()
                finish(w, step - 3)

    drain(WAVES - 1)

    mine = jnp.zeros((8, 128), F32)
    for w in weights:
        for i in range(w.shape[1] // 128):
            mine += squares[w.k][:, 128 * i : 128 * i + 128]
    part_sum[...] = mine

    def tell(k):
        return remote(part_sum, all_sums.at[k - 1], sum_send.at[k - 1], sum_recv.at[k - 1], (me + k) % 16)

    for k in range(1, 16):
        tell(k).start()
    sums = mine
    for k in range(1, 16):
        tell(k).wait_recv()
        sums += all_sums[k - 1]
    sums = jnp.sum(jnp.sum(sums, axis=0, keepdims=True), axis=1, keepdims=True)
    factor = jnp.minimum(1.0, 0.5 * lax.rsqrt(sums / count + 1e-30))

    def update(w, wave):
        layer, cut = w.part(wave)
        here = (layer, *at, core, *cut)
        slot = wave % RING
        g = w_out[w.k][here].astype(F32) * factor
        m = 0.9 * m_own[w.k][slot] + 0.1 * g
        v = 0.95 * v_own[w.k][slot] + 0.05 * g * g
        weight = w_own[w.k][slot].astype(F32)
        w_out[w.k][here] = (weight - 0.02 * (m * lax.rsqrt(v + 1e-8) + 0.1 * weight)).astype(BF16)
        m_own[w.k][slot] = m
        v_own[w.k][slot] = v

    def out_at(w, wave, fixed, which):
        layer, cut = w.part(wave)
        return w_out[w.k].at[(layer, *where(fixed), which, *cut)]

    def give(w, wave, stage):
        slot = wave % SLOTS
        axes = w.axes[::-1]
        ref = out_at(w, wave, {axis: at[axis] for axis in axes[stage:]}, core)
        return remote(ref, ref, gather_send.at[slot, stage, w.k], gather_recv.at[slot, stage, w.k], near[axes[stage]])

    def give_twin(w, wave, half):
        slot = wave % SLOTS
        axis = w.axes[0]
        side = at[axis] if half == 0 else 1 - at[axis]
        ref = out_at(w, wave, {axis: side}, core)
        return remote(ref, ref, back_send.at[slot, half, w.k], back_recv.at[slot, half, w.k], twin)

    def begin(wave):
        for w in weights:
            for copy in fetch(w, wave):
                copy.wait()
            update(w, wave)
            give(w, wave, 0).start()
        for w in weights:
            for copy in put(w, wave):
                copy.start()

    @pl.loop(0, LEAD)
    def _(wave):
        begin(wave)

    @pl.loop(0, WAVES + 5)
    def _(step):
        @pl.when(step >= 5)
        def _():
            for w in weights:
                for stage in range(3):
                    give(w, step - 5, stage).wait_send()
                for half in range(2):
                    give_twin(w, step - 5, half).wait_send()

        @pl.when(step + LEAD < WAVES)
        def _():
            begin(step + LEAD)

        @pl.when(step < WAVES)
        def _():
            for w in weights:
                give(w, step, 0).wait_recv()
                give(w, step, 1).start()

        @pl.when((step >= 1) & (step - 1 < WAVES))
        def _():
            for w in weights:
                give(w, step - 1, 1).wait_recv()
                give(w, step - 1, 2).start()
                give_twin(w, step - 1, 0).start()

        @pl.when((step >= 2) & (step - 2 < WAVES))
        def _():
            for w in weights:
                give(w, step - 2, 2).wait_recv()
                give_twin(w, step - 2, 1).start()

        @pl.when(step < WAVES)
        def _():
            for w in weights:
                for copy in put(w, step):
                    copy.wait()

        @pl.when(step + RING < WAVES)
        def _():
            for w in weights:
                for copy in fetch(w, step + RING):
                    copy.start()

        @pl.when((step >= 4) & (step - 4 < WAVES))
        def _():
            for w in weights:
                for half in range(2):
                    give_twin(w, step - 4, half).wait_recv()

    for k in range(1, 16):
        tell(k).wait_send()


def hand_over(w_from, state, w_to, m_to, v_to, m_by, v_by, sem):
    inward = [pltpu.make_async_copy(state.at[0], m_by, sem.at[0]), pltpu.make_async_copy(state.at[1], v_by, sem.at[1])]
    outward = [pltpu.make_async_copy(m_by, m_to, sem.at[0]), pltpu.make_async_copy(v_by, v_to, sem.at[1])]
    cuts = [(layer, x) for layer in range(LAYERS) for x in range(2)]
    weight = [pltpu.make_async_copy(w_from.at[cut], w_to.at[cut], sem.at[2 + n]) for n, cut in enumerate(cuts)]
    for copy in inward + weight:
        copy.start()
    for copy, back in zip(inward, outward):
        copy.wait()
        back.start()
    for copy in outward + weight:
        copy.wait()


def solution(mesh):
    def step(*arrays):
        terms, whole, m, v = (arrays[i : i + 3] for i in (0, 3, 6, 9))
        weights = [Weight(k, *one.shape[1:]) for k, one in enumerate(m)]
        count = 16 * sum(one.size for one in m)
        cut = [(LAYERS, 2, 2, 2, 2, w.rows, w.columns) for w in weights]
        held = lambda n, extra=(), dtype=BF16: [pltpu.VMEM((n, *extra, *w.shape), dtype) for w in weights]
        scratch = (
            held(HELD, (2, 2))
            + held(HELD, (2,))
            + held(HELD)
            + held(RING)
            + held(RING, dtype=F32)
            + held(RING, dtype=F32)
            + [pltpu.VMEM((8, w.shape[1]), F32) for w in weights]
            + [pltpu.VMEM((8, 128), F32), pltpu.VMEM((15, 8, 128), F32)]
            + [pltpu.SemaphoreType.DMA((SLOTS, 3))] * 3
            + [pltpu.SemaphoreType.DMA((SLOTS, 3, 3))] * 4
            + [pltpu.SemaphoreType.DMA((SLOTS, 2, 3))] * 2
            + [pltpu.SemaphoreType.DMA((RING, 5, 3))]
            + [pltpu.SemaphoreType.DMA((15,))] * 2
        )
        anywhere = pl.BlockSpec(memory_space=pl.ANY)
        out = pl.pallas_call(
            lambda *refs: kernel(weights, float(count), *refs),
            out_shape=[pltpu.VMEM(c, BF16) for c in cut] + [jax.ShapeDtypeStruct((ROOM, *one.shape), F32) for one in m],
            in_specs=[anywhere] * 12,
            out_specs=[pl.BlockSpec(memory_space=pltpu.VMEM)] * 3 + [anywhere] * 3,
            scratch_shapes=scratch,
            compiler_params=pltpu.CompilerParams(collective_id=0, has_side_effects=True, vmem_limit_bytes=GRANT),
            name="step",
        )(*(t.reshape(c) for t, c in zip(terms, cut)), *(t.reshape(c) for t, c in zip(whole, cut)), *m, *v)
        new = [
            pl.pallas_call(
                hand_over,
                out_shape=[jax.ShapeDtypeStruct(cut[w.k], BF16)] + [jax.ShapeDtypeStruct(m[w.k].shape, F32)] * 2,
                in_specs=[pl.BlockSpec(memory_space=pltpu.VMEM), anywhere],
                out_specs=[anywhere] * 3,
                scratch_shapes=[pltpu.VMEM(m[w.k].shape, F32)] * 2 + [pltpu.SemaphoreType.DMA((6,))],
                compiler_params=pltpu.CompilerParams(vmem_limit_bytes=5 * 2**20),
                name="hand_over",
            )(*out[w.k :: 3])
            for w in weights
        ]
        return (*(one[0].reshape(t.shape) for one, t in zip(new, whole)), *(one[1] for one in new), *(one[2] for one in new))

    all_of, cut = P(None, None, None), P(None, "dp", None)
    return jax.shard_map(
        step,
        mesh=mesh,
        in_specs=(P(("rep", "dp"), None, None, None),) * 3 + (all_of,) * 3 + (cut,) * 6,
        out_specs=(P("rep", None, None),) * 3 + (P("rep", "dp", None),) * 6,
        check_vma=False,
    )
```
